16 devices in a mesh: dp: 4 (over y, z, core), tp: 4 (over x).
Axes of the slice: x: 4, y: 2, z: 1, core: 2. Of those that a mesh axis runs over, the one named last changes fastest.
The devices are a block of a 4x4x4 slice.
Arguments:
- x: bfloat16 [2048, 12288], P(('dp', 'tp')), parts along dimension 0
- gain_a: bfloat16 [12288], replicated
- wq: bfloat16 [12288, 12288], P(None, 'tp')
- wk: bfloat16 [12288, 1024], P(None, 'tp')
- wv: bfloat16 [12288, 1024], P(None, 'tp')
- wo: bfloat16 [12288, 12288], P('tp')
- gain_m: bfloat16 [12288], replicated
- w_gate: bfloat16 [12288, 33792], P(None, 'tp')
- w_up: bfloat16 [12288, 33792], P(None, 'tp')
- w_down: bfloat16 [33792, 12288], P('tp')
Outputs:
- output: bfloat16 [2048, 12288], P(('dp', 'tp')), parts along dimension 0
There are 4 independent parts. The reference program is written for one: setup_inputs(seed, part) draws one part's arguments, and reference() takes and returns one part's arrays. A program takes and returns all parts, laid end to end along the dimension named above; an argument that names none is the same for every part.
All inputs are finite; a program needn't handle non-finite values.
Results may differ from the reference program's by a relative error of at most 0.017.
Values are sent between devices in bfloat16 or wider.
A program may use at most 1.5 GiB of HBM per device.

```python
import jax
import jax.numpy as jnp
from jax import lax

ROWS = 512
D = 12288
HEADS = 96
KV_HEADS = 8
HEAD = 128
FF = 33792
THETA = 10000


def setup_inputs(seed: int = 0, part: int = 0) -> dict:
    kx, kn, kq, kk, kv, ko, km, kg, ku, kd = jax.random.split(jax.random.key(seed), 10)

    def weights(key, rows, columns):
        return jax.random.normal(key, (rows, columns), jnp.float32) * rows**-0.5

    drawn = {
        "x": jax.random.normal(jax.random.fold_in(kx, part), (ROWS, D), jnp.float32),
        "gain_a": 1 + 0.1 * jax.random.normal(kn, (D,), jnp.float32),
        "wq": 2 * weights(kq, D, HEADS * HEAD),
        "wk": 2 * weights(kk, D, KV_HEADS * HEAD),
        "wv": 4 * weights(kv, D, KV_HEADS * HEAD),
        "wo": weights(ko, HEADS * HEAD, D),
        "gain_m": 1 + 0.1 * jax.random.normal(km, (D,), jnp.float32),
        "w_gate": weights(kg, D, FF),
        "w_up": weights(ku, D, FF),
        "w_down": 2 * weights(kd, FF, D),
    }
    return {k: v.astype(jnp.bfloat16) for k, v in drawn.items()}


def normed(x, gain):
    wide = x.astype(jnp.float32)
    scale = lax.rsqrt(jnp.mean(wide * wide, -1, keepdims=True) + 1e-6)
    return (wide * scale * gain.astype(jnp.float32)).astype(jnp.bfloat16)


def turned(t, place, theta):
    half = t.shape[-1] // 2
    angle = place.astype(jnp.float32)[:, None] * theta ** (-jnp.arange(half, dtype=jnp.float32) / half)
    cos, sin = jnp.cos(angle)[:, None], jnp.sin(angle)[:, None]
    a, b = t[..., :half].astype(jnp.float32), t[..., half:].astype(jnp.float32)
    return jnp.concatenate([a * cos - b * sin, b * cos + a * sin], -1).astype(jnp.bfloat16)


def matmul(a, w):
    return jnp.dot(a, w, preferred_element_type=jnp.float32).astype(jnp.bfloat16)


def einsum(form, a, b):
    return jnp.einsum(form, a.astype(jnp.float32), b.astype(jnp.float32))


def attention(q, k, v):
    scores = einsum("tgsd,ugd->gstu", q, k) * q.shape[-1] ** -0.5
    token = jnp.arange(q.shape[0])
    scores = jnp.where(token[:, None] >= token, scores, -jnp.inf)
    weights = jax.nn.softmax(scores, -1).astype(jnp.bfloat16)
    return einsum("gstu,ugd->tgsd", weights, v).astype(jnp.bfloat16)


def reference(x, gain_a, wq, wk, wv, wo, gain_m, w_gate, w_up, w_down):
    a, place = normed(x, gain_a), jnp.arange(ROWS)
    q = turned(matmul(a, wq).reshape(ROWS, HEADS, HEAD), place, THETA).reshape(ROWS, KV_HEADS, -1, HEAD)
    k = turned(matmul(a, wk).reshape(ROWS, KV_HEADS, HEAD), place, THETA)
    v = matmul(a, wv).reshape(ROWS, KV_HEADS, HEAD)
    seen = attention(q, k, v).reshape(ROWS, HEADS * HEAD)
    h = (x.astype(jnp.float32) + jnp.dot(seen, wo, preferred_element_type=jnp.float32)).astype(jnp.bfloat16)
    b = normed(h, gain_m)
    gate = jnp.dot(b, w_gate, preferred_element_type=jnp.float32)
    up = jnp.dot(b, w_up, preferred_element_type=jnp.float32)
    hidden = (jax.nn.silu(gate) * up).astype(jnp.bfloat16)
    return (h.astype(jnp.float32) + jnp.dot(hidden, w_down, preferred_element_type=jnp.float32)).astype(jnp.bfloat16)
```

```python
import functools

import jax
import jax.numpy as jnp
import numpy as np
from jax import lax
from jax.experimental import pallas as pl
from jax.experimental.pallas import tpu as pltpu
from jax.sharding import PartitionSpec as P

HEAD = 128
THETA = 10000
LOG2E = 1.4426950408889634
VMEM = 67043328
MESH = pl.DeviceIdType.MESH
F32, BF16 = jnp.float32, jnp.bfloat16


def _fit(size, want):
    return max(n for n in range(128, want + 1, 128) if size % n == 0)


def _whole(shape):
    return pl.BlockSpec(shape, lambda *_: (0,) * len(shape), pipeline_mode=pl.Buffered(1))


def _ring(n):
    me = lax.axis_index("tp")
    return me, lax.rem(me + 1, n), lax.rem(me + n - 1, n), lax.rem(me + n // 2, n)


def _greet(left, right):
    barrier = pltpu.get_barrier_semaphore()
    for neighbour in (left, right):
        pl.semaphore_signal(barrier, inc=1, device_id={"tp": neighbour}, device_id_type=MESH)


def _met():
    pl.semaphore_wait(pltpu.get_barrier_semaphore(), 2)


def _copy(src, dst, send, recv, to):
    return pltpu.make_async_remote_copy(src_ref=src, dst_ref=dst, send_sem=send, recv_sem=recv, device_id={"tp": to}, device_id_type=MESH)


class _Gather:
    def __init__(self, n, all_s, send, recv):
        self.n, self.all_s, self.send, self.recv = n, all_s, send, recv
        self.chunks, self.rows = all_s.shape[0], all_s.shape[1] // n
        self.me, self.right, self.left, self.far = _ring(n)

    def part(self, j, owner, half=None):
        rows = self.rows if half is None else self.rows // 2
        start = owner * self.rows + (0 if half is None else half * rows)
        return self.all_s.at[j, pl.ds(pl.multiple_of(start, rows), rows), :]

    def copy(self, kind, j, arriving=False):
        to = self.right if kind % 2 == 0 else self.left
        if kind < 2:
            owner = (self.left if kind == 0 else self.right) if arriving else self.me
            at = self.part(j, owner)
        else:
            owner = self.far if arriving else (self.left if kind == 2 else self.right)
            at = self.part(j, owner, kind - 2)
        return _copy(at, at, self.send.at[kind, j], self.recv.at[kind, j], to)

    def direct(self, j):
        @pl.when(j < self.chunks)
        def _():
            for kind in (0, 1):
                self.copy(kind, j).start()

    def forward(self, j):
        for kind in (0, 1):
            self.copy(kind, j, True).wait_recv()
            self.copy(kind + 2, j).start()

    def arrived(self, j):
        for kind in (2, 3):
            self.copy(kind, j, True).wait_recv()

    def sent(self):
        def one(j, _):
            for kind in range(4):
                self.copy(kind, j).wait_send()

        lax.fori_loop(0, self.chunks, one, None)

    def scale(self, x_ref):
        rows, width = x_ref.shape
        wide = self.all_s.shape[2]

        def squares(j, total):
            for i in range(wide // 128):
                t = x_ref[:, pl.ds(pl.multiple_of(j * wide + i * 128, 128), 128)].astype(F32)
                total = total + t * t
            return total

        total = lax.fori_loop(0, self.chunks, squares, jnp.zeros((rows, 128), F32))
        return lax.rsqrt(total.sum(-1, keepdims=True) / width + 1e-6)

    def open(self, x_ref, gain_ref, layer, eager):
        _greet(self.left, self.right)
        scale = self.scale(x_ref)
        rows, wide = self.rows, self.all_s.shape[2]
        mine = pl.ds(pl.multiple_of(self.me * rows, rows), rows)

        def one(j, _):
            here = pl.ds(pl.multiple_of(j * wide, wide), wide)
            self.all_s[j, mine, :] = (x_ref[:, here].astype(F32) * scale * gain_ref[layer : layer + 1, here].astype(F32)).astype(BF16)

        one(0, None)
        _met()
        self.direct(0)
        lax.fori_loop(1, self.chunks, one, None)
        if eager:
            self.direct(1)
        self.forward(0)
        if not eager:
            self.direct(1)
        self.direct(2)

    def step(self, c):
        @pl.when(c + 1 < self.chunks)
        def _():
            self.forward(c + 1)
            self.direct(c + 3)

        self.arrived(c)


def _dot(a, b):
    return jnp.dot(a, b, preferred_element_type=F32)


def _project(n, x_ref, gain_ref, wq_ref, wk_ref, wv_ref, cos_ref, sin_ref, q_ref, k_ref, v_ref, all_s, q_s, k_s, v_s, send, recv):
    c = pl.program_id(0)
    g = _Gather(n, all_s, send, recv)

    @pl.when(c == 0)
    def _():
        q_s[...] = jnp.zeros_like(q_s)
        k_s[...] = jnp.zeros_like(k_s)
        v_s[...] = jnp.zeros_like(v_s)
        g.open(x_ref, gain_ref, 0, True)

    g.step(c)
    wide = _fit(q_s.shape[1], 768)
    for at in range(0, q_s.shape[1], wide):
        q_s[:, at : at + wide] += _dot(all_s[c], wq_ref[:, at : at + wide])
    k_s[...] += _dot(all_s[c], wk_ref[...])
    v_s[...] += _dot(all_s[c], wv_ref[...])

    @pl.when(c == g.chunks - 1)
    def _():
        def turned(t):
            t = t.astype(BF16).astype(F32)
            return (t * cos_ref[...] + pltpu.roll(t, HEAD // 2, 1) * sin_ref[...]).astype(BF16)

        def head(i, _):
            here = pl.ds(pl.multiple_of(i * HEAD, HEAD), HEAD)
            q_ref[:, here] = turned(q_s[:, here])

        lax.fori_loop(0, q_s.shape[1] // HEAD, head, None)
        for at in range(0, k_s.shape[1], HEAD):
            k_ref[:, at : at + HEAD] = turned(k_s[:, at : at + HEAD])
        v_ref[...] = v_s[...].astype(BF16)
        g.sent()


def _place(s, chunks, tiles, early):
    late = s - early * chunks
    return (jnp.where(late < 0, lax.div(s, early), lax.rem(jnp.maximum(late, 0), chunks)),
            jnp.where(late < 0, lax.rem(s, early), early + lax.div(jnp.maximum(late, 0), chunks)))


def _gate_up(n, tiles, early, x_ref, gain_ref, wg_ref, wu_ref, out_ref, all_s, g_s, u_s, send, recv):
    s = pl.program_id(0)
    g = _Gather(n, all_s, send, recv)
    c, t = _place(s, g.chunks, tiles, early)
    slot = jnp.where(t < early, t, 0)

    @pl.when(s == 0)
    def _():
        g.open(x_ref, gain_ref, 1, False)

    @pl.when((s < early * g.chunks) & (t == 0))
    def _():
        g.step(c)

    @pl.when(c == 0)
    def _():
        g_s[slot] = _dot(all_s[c], wg_ref[...])
        u_s[slot] = _dot(all_s[c], wu_ref[...])

    @pl.when((c > 0) & (c < g.chunks - 1))
    def _():
        for at in range(0, wg_ref.shape[1], 256):
            here = slice(at, at + 256)
            g_s[slot, :, here] += _dot(all_s[c], wg_ref[:, here])
            u_s[slot, :, here] += _dot(all_s[c], wu_ref[:, here])

    @pl.when(c == g.chunks - 1)
    def _():
        for at in range(0, wg_ref.shape[1], 256):
            here = slice(at, at + 256)
            gate = g_s[slot, :, here] + _dot(all_s[c], wg_ref[:, here])
            up = u_s[slot, :, here] + _dot(all_s[c], wu_ref[:, here])
            out_ref[:, here] = (gate / (1 + jnp.exp(-gate)) * up).astype(BF16)

    @pl.when(s == pl.num_programs(0) - 1)
    def _():
        g.sent()


def _gather_scratch(n, rows, width, wide):
    chunks = width // wide
    return [pltpu.VMEM((chunks, n * rows, wide), BF16)], [pltpu.SemaphoreType.DMA((4, chunks))] * 2


def project(n, x, gains, wq, wk, wv, cos, sin, wide=768):
    rows, width = x.shape
    wide = _fit(width, wide)
    first, last = _gather_scratch(n, rows, width, wide)
    tokens, nq, nk = n * rows, wq.shape[1], wk.shape[1]
    weight = lambda w: pl.BlockSpec((wide, w.shape[1]), lambda c: (c, 0))
    return pl.pallas_call(
        functools.partial(_project, n),
        grid=(width // wide,),
        in_specs=[_whole(x.shape), _whole(gains.shape), weight(wq), weight(wk), weight(wv), _whole(cos.shape), _whole(sin.shape)],
        out_specs=[_whole((tokens, nq)), _whole((tokens, nk)), _whole((tokens, nk))],
        out_shape=[jax.ShapeDtypeStruct((tokens, w), BF16) for w in (nq, nk, nk)],
        scratch_shapes=[*first, *(pltpu.VMEM((tokens, w), F32) for w in (nq, nk, nk)), *last],
        compiler_params=pltpu.CompilerParams(collective_id=0, has_side_effects=True, vmem_limit_bytes=VMEM, dimension_semantics=("arbitrary",)),
        cost_estimate=pl.CostEstimate(flops=2 * tokens * width * (nq + 2 * nk), transcendentals=0, bytes_accessed=2 * width * (nq + 2 * nk)),
        name="project",
    )(x, gains, wq, wk, wv, cos, sin)


def gate_up(n, x, gains, w_gate, w_up, wide=768, tile=2816):
    rows, width = x.shape
    hidden = w_gate.shape[1]
    wide, tile = _fit(width, wide), _fit(hidden, tile)
    first, last = _gather_scratch(n, rows, width, wide)
    tokens, chunks, tiles = n * rows, width // wide, hidden // tile
    early = tiles - tiles // 3
    weight = pl.BlockSpec((wide, tile), lambda s: _place(s, chunks, tiles, early))

    def done(s):
        c, t = _place(s, chunks, tiles, early)
        return 0, jnp.where((t < early) & (c < chunks - 1), 0, t)

    return pl.pallas_call(
        functools.partial(_gate_up, n, tiles, early),
        grid=(chunks * tiles,),
        in_specs=[_whole(x.shape), _whole(gains.shape), weight, weight],
        out_specs=pl.BlockSpec((tokens, tile), done, pipeline_mode=pl.Buffered(1)),
        out_shape=jax.ShapeDtypeStruct((tokens, hidden), BF16),
        scratch_shapes=[*first, *[pltpu.VMEM((early, tokens, tile), F32)] * 2, *last],
        compiler_params=pltpu.CompilerParams(collective_id=1, has_side_effects=True, vmem_limit_bytes=VMEM, dimension_semantics=("arbitrary",)),
        cost_estimate=pl.CostEstimate(flops=4 * tokens * width * hidden, transcendentals=tokens * hidden, bytes_accessed=4 * width * hidden),
        name="gate_up",
    )(x, gains, w_gate, w_up)


def _scatter(n, chunks, lags, a_ref, w_ref, x_ref, y_ref, made_s, far_s, to_s, far_in, from_in, send, recv):
    c = pl.program_id(0)
    me, right, left, far = _ring(n)
    rows, slots = x_ref.shape[0], made_s.shape[0]
    half = rows // 2
    on, last = c - lags[0], c - lags[1]

    def block(j, owner, start=0, size=rows):
        return made_s[lax.rem(j, slots), pl.ds(pl.multiple_of(owner * rows + start, half), size), :]

    def far_copy(way, j):
        return _copy(far_s.at[j, way], far_in.at[j, way], send.at[way, j], recv.at[way, j], (right, left)[way])

    def to_copy(way, j):
        return _copy(to_s.at[way, j], from_in.at[way, j], send.at[way + 2, j], recv.at[way + 2, j], (right, left)[way])

    def make():
        made_s[lax.rem(c, slots)] = _dot(a_ref[...], w_ref[...])

    def set_off():
        for way in (0, 1):
            far_s[c, way] = block(c, far, way * half, half).astype(BF16)
        for way in (0, 1):
            far_copy(way, c).start()

    def pass_on(way):
        to = (right, left)[way]
        mixed, plain = way * half, (1 - way) * half
        to_s[way, on, plain : plain + half, :] = block(on, to, plain, half).astype(BF16)
        to_s[way, on, mixed : mixed + half, :] = (block(on, to, mixed, half) + far_in[on, way].astype(F32)).astype(BF16)

    def finish():
        total = block(last, me) + from_in[0, last].astype(F32) + from_in[1, last].astype(F32)
        y_ref[...] = (x_ref[...].astype(F32) + total).astype(BF16)

    steady = (last >= 0) & (c < chunks)
    if lags[0] == 1:
        steady = c < 0

    @pl.when(c == 0)
    def _():
        _greet(left, right)

    @pl.when((c < chunks) & jnp.logical_not(steady))
    def _():
        make()

        @pl.when(c == 0)
        def _():
            _met()

        set_off()

    if lags[0] > 1:

        @pl.when(steady)
        def _():
            for way in (0, 1):
                far_copy(way, on).wait_recv()
                to_copy(way, last).wait_recv()
            for way in (0, 1):
                pass_on(way)
            finish()
            make()
            for way in (0, 1):
                to_copy(way, on).start()
            set_off()

    @pl.when((on >= 0) & (on < chunks) & jnp.logical_not(steady))
    def _():
        for way in (0, 1):
            far_copy(way, on).wait_recv()
            pass_on(way)
            to_copy(way, on).start()

    @pl.when((last >= 0) & jnp.logical_not(steady))
    def _():
        for way in (0, 1):
            to_copy(way, last).wait_recv()
        finish()

    @pl.when(c == pl.num_programs(0) - 1)
    def _():
        def one(j, _):
            for way in (0, 1):
                far_copy(way, j).wait_send()
                to_copy(way, j).wait_send()

        lax.fori_loop(0, chunks, one, None)


def scatter(n, a, w, x, wide, lags, ident, name):
    (tokens, depth), width = a.shape, w.shape[1]
    rows = tokens // n
    wide = _fit(width, wide)
    chunks = width // wide
    done = pl.BlockSpec((rows, wide), lambda c: (0, jnp.maximum(c - lags[1], 0)))
    return pl.pallas_call(
        functools.partial(_scatter, n, chunks, lags),
        grid=(chunks + lags[1],),
        in_specs=[_whole(a.shape), pl.BlockSpec((depth, wide), lambda c: (0, jnp.minimum(c, chunks - 1))), done],
        out_specs=done,
        out_shape=jax.ShapeDtypeStruct((rows, width), BF16),
        scratch_shapes=[
            pltpu.VMEM((lags[1] + 1, tokens, wide), F32),
            pltpu.VMEM((chunks, 2, rows // 2, wide), BF16),
            pltpu.VMEM((2, chunks, rows, wide), BF16),
            pltpu.VMEM((chunks, 2, rows // 2, wide), BF16),
            pltpu.VMEM((2, chunks, rows, wide), BF16),
            pltpu.SemaphoreType.DMA((4, chunks)),
            pltpu.SemaphoreType.DMA((4, chunks)),
        ],
        compiler_params=pltpu.CompilerParams(collective_id=ident, has_side_effects=True, vmem_limit_bytes=VMEM, dimension_semantics=("arbitrary",)),
        cost_estimate=pl.CostEstimate(flops=2 * tokens * width * depth, transcendentals=0, bytes_accessed=2 * width * depth),
        name=name,
    )(a, w, x)


def _attend(heads, q_ref, k_ref, v_ref, o_ref, v_s):
    tokens = q_ref.shape[0]
    e = HEAD**-0.5 * LOG2E
    v_s[:, :HEAD] = v_ref[...]
    v_s[:, HEAD:] = jnp.ones((tokens, HEAD), BF16)
    size, cols = HEAD, [slice(i * HEAD, (i + 1) * HEAD) for i in range(heads)]
    shape = (heads * size, size)
    seen = lax.rem(lax.broadcasted_iota(jnp.int32, shape, 0), size) >= lax.broadcasted_iota(jnp.int32, shape, 1)
    for at in range(0, tokens, size):
        end = at + size
        q = jnp.concatenate([q_ref[at:end, c] for c in cols], axis=0)
        s = lax.dot_general(q, k_ref[:end, :], (((1,), (1,)), ((), ())), preferred_element_type=F32)
        last = jnp.where(seen, s[:, at:], -jnp.inf)
        s = jnp.concatenate([s[:, :at], last], axis=1) if at else last
        top = s.max(-1, keepdims=True)
        p = jnp.exp2((s - top) * e).astype(BF16)
        mix = _dot(p, v_s[:end, :])
        out = (mix[:, :HEAD] / mix[:, HEAD:]).astype(BF16)
        for i, c in enumerate(cols):
            o_ref[at:end, c] = out[i * size : (i + 1) * size]


def attention(q, k, v, heads=4):
    tokens, width = q.shape
    per = width // k.shape[1] // heads
    key = pl.BlockSpec((tokens, HEAD), lambda i: (0, i // per))
    query = pl.BlockSpec((tokens, heads * HEAD), lambda i: (0, i))
    return pl.pallas_call(
        functools.partial(_attend, heads),
        grid=(width // HEAD // heads,),
        in_specs=[query, key, key],
        out_specs=query,
        out_shape=jax.ShapeDtypeStruct(q.shape, BF16),
        scratch_shapes=[pltpu.VMEM((tokens, 2 * HEAD), BF16)],
        compiler_params=pltpu.CompilerParams(dimension_semantics=("arbitrary",), vmem_limit_bytes=VMEM),
        cost_estimate=pl.CostEstimate(flops=4 * tokens * tokens * width, transcendentals=tokens * tokens * width // HEAD, bytes_accessed=4 * q.size),
        name="attention",
    )(q, k, v)


def rotation(tokens):
    half = HEAD // 2
    angle = np.arange(tokens, dtype=np.float32)[:, None] * np.float32(THETA) ** (-np.arange(half, dtype=np.float32) / np.float32(half))
    cos, sin = np.cos(angle), np.sin(angle)
    return np.concatenate([cos, cos], 1).astype(np.float32), np.concatenate([-sin, sin], 1).astype(np.float32)


def solution(mesh):
    n = mesh.shape["tp"]

    def step(x, gain_a, wq, wk, wv, wo, gain_m, w_gate, w_up, w_down):
        cos, sin = rotation(n * x.shape[0])
        shape = (2, x.shape[1])
        gains = jnp.where(lax.broadcasted_iota(jnp.int32, shape, 0) == 0, *(lax.broadcast_in_dim(t, shape, (1,)) for t in (gain_a, gain_m)))
        q, k, v = project(n, x, gains, wq, wk, wv, jnp.asarray(cos), jnp.asarray(sin))
        h = scatter(n, attention(q, k, v), wo, x, 768, (1, 2), 2, "attention_out")
        hidden = gate_up(n, h, gains, w_gate, w_up)
        return scatter(n, hidden, w_down, h, 512, (2, 4), 3, "down")

    tokens, columns, rows_of = P(("dp", "tp"), None), P(None, "tp"), P("tp", None)
    return jax.shard_map(
        step,
        mesh=mesh,
        in_specs=(tokens, P(None), columns, columns, columns, rows_of, P(None), columns, columns, rows_of),
        out_specs=tokens,
        check_vma=False,
    )
```

```python
import functools

import jax
import jax.numpy as jnp
import numpy as np
from jax import lax
from jax.experimental import pallas as pl
from jax.experimental.pallas import tpu as pltpu
from jax.sharding import PartitionSpec as P

HEAD = 128
THETA = 10000
LOG2E = 1.4426950408889634
VMEM = 67043328
MESH = pl.DeviceIdType.MESH
F32, BF16 = jnp.float32, jnp.bfloat16


def _fit(size, want):
    return max(n for n in range(128, want + 1, 128) if size % n == 0)


def _whole(shape):
    return pl.BlockSpec(shape, lambda *_: (0,) * len(shape), pipeline_mode=pl.Buffered(1))


def _ring(n):
    me = lax.axis_index("tp")
    return me, lax.rem(me + 1, n), lax.rem(me + n - 1, n), lax.rem(me + n // 2, n)


def _greet(left, right):
    barrier = pltpu.get_barrier_semaphore()
    for neighbour in (left, right):
        pl.semaphore_signal(barrier, inc=1, device_id={"tp": neighbour}, device_id_type=MESH)


def _met():
    pl.semaphore_wait(pltpu.get_barrier_semaphore(), 2)


def _copy(src, dst, send, recv, to):
    return pltpu.make_async_remote_copy(src_ref=src, dst_ref=dst, send_sem=send, recv_sem=recv, device_id={"tp": to}, device_id_type=MESH)


class _Gather:
    def __init__(self, n, all_s, send, recv):
        self.n, self.all_s, self.send, self.recv = n, all_s, send, recv
        self.chunks, self.rows = all_s.shape[0], all_s.shape[1] // n
        self.me, self.right, self.left, self.far = _ring(n)

    def part(self, j, owner, half=None):
        rows = self.rows if half is None else self.rows // 2
        start = owner * self.rows + (0 if half is None else half * rows)
        return self.all_s.at[j, pl.ds(pl.multiple_of(start, rows), rows), :]

    def copy(self, kind, j, arriving=False):
        to = self.right if kind % 2 == 0 else self.left
        if kind < 2:
            owner = (self.left if kind == 0 else self.right) if arriving else self.me
            at = self.part(j, owner)
        else:
            owner = self.far if arriving else (self.left if kind == 2 else self.right)
            at = self.part(j, owner, kind - 2)
        return _copy(at, at, self.send.at[kind, j], self.recv.at[kind, j], to)

    def direct(self, j):
        @pl.when(j < self.chunks)
        def _():
            for kind in (0, 1):
                self.copy(kind, j).start()

    def forward(self, j):
        for kind in (0, 1):
            self.copy(kind, j, True).wait_recv()
            self.copy(kind + 2, j).start()

    def arrived(self, j):
        for kind in (2, 3):
            self.copy(kind, j, True).wait_recv()

    def sent(self):
        def one(j, _):
            for kind in range(4):
                self.copy(kind, j).wait_send()

        lax.fori_loop(0, self.chunks, one, None)

    def scale(self, x_ref):
        rows, width = x_ref.shape
        wide = self.all_s.shape[2]

        def squares(j, total):
            for i in range(wide // 128):
                t = x_ref[:, pl.ds(pl.multiple_of(j * wide + i * 128, 128), 128)].astype(F32)
                total = total + t * t
            return total

        total = lax.fori_loop(0, self.chunks, squares, jnp.zeros((rows, 128), F32))
        return lax.rsqrt(total.sum(-1, keepdims=True) / width + 1e-6)

    def open(self, x_ref, gain_ref, gain_s, scale, eager, between=None):
        gain_s[...] = gain_ref[...].astype(F32)
        scale = self.scale(x_ref) if scale is None else scale
        rows, wide = self.rows, self.all_s.shape[2]
        mine = pl.ds(pl.multiple_of(self.me * rows, rows), rows)

        def one(j, _):
            for i in range(wide // 128):
                t = x_ref[:, pl.ds(pl.multiple_of(j * wide + i * 128, 128), 128)].astype(F32)
                self.all_s[j, mine, i * 128 : (i + 1) * 128] = (t * scale * gain_s[pl.ds(j * (wide // 128) + i, 1), :]).astype(BF16)

        one(0, None)
        _met()
        self.direct(0)
        if eager:
            one(1, None)
            self.direct(1)
        lax.fori_loop(1 + eager, self.chunks, one, None)
        if between:
            between()
        self.forward(0)
        if not eager:
            self.direct(1)
        self.direct(2)

    def step(self, c):
        @pl.when(c + 1 < self.chunks)
        def _():
            self.forward(c + 1)
            self.direct(c + 3)

        self.arrived(c)


def _dot(a, b):
    return jnp.dot(a, b, preferred_element_type=F32)


def _project(n, x_ref, gain_ref, wq_ref, wk_ref, wv_ref, cos_ref, sin_ref, q_ref, k_ref, v_ref, all_s, gain_s, q_s, k_s, v_s, send, recv):
    c = pl.program_id(0)
    g = _Gather(n, all_s, send, recv)

    @pl.when(c == 0)
    def _():
        def clear():
            for t in (q_s, k_s, v_s):
                t[...] = jnp.zeros_like(t)

        _greet(g.left, g.right)
        g.open(x_ref, gain_ref, gain_s, None, True, clear)

    g.step(c)
    wide = _fit(q_s.shape[1], 768)
    for at in range(0, q_s.shape[1], wide):
        q_s[:, at : at + wide] += _dot(all_s[c], wq_ref[:, at : at + wide])
    k_s[...] += _dot(all_s[c], wk_ref[...])
    v_s[...] += _dot(all_s[c], wv_ref[...])

    @pl.when(c == g.chunks - 1)
    def _():
        def turned(t):
            t = t.astype(BF16).astype(F32)
            return (t * cos_ref[...] + pltpu.roll(t, HEAD // 2, 1) * sin_ref[...]).astype(BF16)

        def head(i, _):
            here = pl.ds(pl.multiple_of(i * HEAD, HEAD), HEAD)
            q_ref[:, here] = turned(q_s[:, here])

        lax.fori_loop(0, q_s.shape[1] // HEAD, head, None)
        for at in range(0, k_s.shape[1], HEAD):
            k_ref[:, at : at + HEAD] = turned(k_s[:, at : at + HEAD])
        v_ref[...] = v_s[...].astype(BF16)
        g.sent()


def _place(s, chunks, tiles, early):
    late = s - early * chunks
    return (jnp.where(late < 0, lax.div(s, early), lax.rem(jnp.maximum(late, 0), chunks)),
            jnp.where(late < 0, lax.rem(s, early), early + lax.div(jnp.maximum(late, 0), chunks)))


def _gate_up(n, tiles, early, x_ref, scale_ref, gain_ref, wg_ref, wu_ref, out_ref, all_s, gain_s, g_s, u_s, send, recv):
    s = pl.program_id(0)
    g = _Gather(n, all_s, send, recv)
    c, t = _place(s, g.chunks, tiles, early)
    slot = jnp.where(t < early, t, 0)

    @pl.when(s == 0)
    def _():
        _greet(g.left, g.right)
        g.open(x_ref, gain_ref, gain_s, scale_ref[...], False)

    @pl.when((s < early * g.chunks) & (t == 0))
    def _():
        g.step(c)

    @pl.when(c == 0)
    def _():
        g_s[slot] = _dot(all_s[c], wg_ref[...])
        u_s[slot] = _dot(all_s[c], wu_ref[...])

    @pl.when((c > 0) & (c < g.chunks - 1))
    def _():
        for at in range(0, wg_ref.shape[1], 256):
            here = slice(at, at + 256)
            g_s[slot, :, here] += _dot(all_s[c], wg_ref[:, here])
            u_s[slot, :, here] += _dot(all_s[c], wu_ref[:, here])

    @pl.when(c == g.chunks - 1)
    def _():
        for at in range(0, wg_ref.shape[1], 256):
            here = slice(at, at + 256)
            gate = g_s[slot, :, here] + _dot(all_s[c], wg_ref[:, here])
            up = u_s[slot, :, here] + _dot(all_s[c], wu_ref[:, here])
            out_ref[:, here] = (gate / (1 + jnp.exp(-gate)) * up).astype(BF16)

    @pl.when(s == pl.num_programs(0) - 1)
    def _():
        g.sent()


def _gather_scratch(n, rows, width, wide):
    chunks = width // wide
    return [pltpu.VMEM((chunks, n * rows, wide), BF16), pltpu.VMEM((width // 128, 128), F32)], [pltpu.SemaphoreType.DMA((4, chunks))] * 2


def project(n, x, gain, wq, wk, wv, cos, sin, wide=512):
    rows, width = x.shape
    wide = _fit(width, wide)
    first, last = _gather_scratch(n, rows, width, wide)
    tokens, nq, nk = n * rows, wq.shape[1], wk.shape[1]
    weight = lambda w: pl.BlockSpec((wide, w.shape[1]), lambda c: (c, 0))
    return pl.pallas_call(
        functools.partial(_project, n),
        grid=(width // wide,),
        in_specs=[_whole(x.shape), _whole((width // 128, 128)), weight(wq), weight(wk), weight(wv), _whole(cos.shape), _whole(sin.shape)],
        out_specs=[_whole((tokens, nq)), _whole((tokens, nk)), _whole((tokens, nk))],
        out_shape=[jax.ShapeDtypeStruct((tokens, w), BF16) for w in (nq, nk, nk)],
        scratch_shapes=[*first, *(pltpu.VMEM((tokens, w), F32) for w in (nq, nk, nk)), *last],
        compiler_params=pltpu.CompilerParams(collective_id=0, has_side_effects=True, vmem_limit_bytes=VMEM, dimension_semantics=("arbitrary",)),
        cost_estimate=pl.CostEstimate(flops=2 * tokens * width * (nq + 2 * nk), transcendentals=0, bytes_accessed=2 * width * (nq + 2 * nk)),
        name="project",
    )(x, gain.reshape(-1, 128), wq, wk, wv, cos, sin)


def gate_up(n, x, scale, gain, w_gate, w_up, wide=768, tile=2816):
    rows, width = x.shape
    hidden = w_gate.shape[1]
    wide, tile = _fit(width, wide), _fit(hidden, tile)
    first, last = _gather_scratch(n, rows, width, wide)
    tokens, chunks, tiles = n * rows, width // wide, hidden // tile
    early = tiles - tiles // 3
    weight = pl.BlockSpec((wide, tile), lambda s: _place(s, chunks, tiles, early))

    def done(s):
        c, t = _place(s, chunks, tiles, early)
        return 0, jnp.where((t < early) & (c < chunks - 1), 0, t)

    return pl.pallas_call(
        functools.partial(_gate_up, n, tiles, early),
        grid=(chunks * tiles,),
        in_specs=[_whole(x.shape), _whole(scale.shape), _whole((width // 128, 128)), weight, weight],
        out_specs=pl.BlockSpec((tokens, tile), done, pipeline_mode=pl.Buffered(1)),
        out_shape=jax.ShapeDtypeStruct((tokens, hidden), BF16),
        scratch_shapes=[*first, *[pltpu.VMEM((early, tokens, tile), F32)] * 2, *last],
        compiler_params=pltpu.CompilerParams(collective_id=1, has_side_effects=True, vmem_limit_bytes=VMEM, dimension_semantics=("arbitrary",)),
        cost_estimate=pl.CostEstimate(flops=4 * tokens * width * hidden, transcendentals=tokens * hidden, bytes_accessed=4 * width * hidden),
        name="gate_up",
    )(x, scale, gain.reshape(-1, 128), w_gate, w_up)


def _scatter(n, chunks, lags, a_ref, w_ref, x_ref, y_ref, scale_ref, square_s, made_s, far_s, to_s, far_in, from_in, send, recv):
    c = pl.program_id(0)
    me, right, left, far = _ring(n)
    rows, slots = x_ref.shape[0], made_s.shape[0]
    half = rows // 2
    on, last = c - lags[0], c - lags[1]

    def block(j, owner, start=0, size=rows):
        return made_s[lax.rem(j, slots), pl.ds(pl.multiple_of(owner * rows + start, half), size), :]

    def far_copy(way, j):
        return _copy(far_s.at[j, way], far_in.at[j, way], send.at[way, j], recv.at[way, j], (right, left)[way])

    def to_copy(way, j):
        return _copy(to_s.at[way, j], from_in.at[way, j], send.at[way + 2, j], recv.at[way + 2, j], (right, left)[way])

    def make():
        made_s[lax.rem(c, slots)] = _dot(a_ref[...], w_ref[...])

    def set_off():
        for way in (0, 1):
            far_s[c, way] = block(c, far, way * half, half).astype(BF16)
        for way in (0, 1):
            far_copy(way, c).start()

    def pass_on(way, on):
        to = (right, left)[way]
        mixed, plain = way * half, (1 - way) * half
        to_s[way, on, plain : plain + half, :] = block(on, to, plain, half).astype(BF16)
        to_s[way, on, mixed : mixed + half, :] = (block(on, to, mixed, half) + far_in[on, way].astype(F32)).astype(BF16)

    def pass_through(j):
        for way in (0, 1):
            far_copy(way, j).wait_recv()
            pass_on(way, j)
            to_copy(way, j).start()

    def finish():
        total = block(last, me) + from_in[0, last].astype(F32) + from_in[1, last].astype(F32)
        y = (x_ref[...].astype(F32) + total).astype(BF16)
        y_ref[...] = y
        if lags[0] == 1:
            y = y.astype(F32)
            square_s[...] += sum(y[:, at : at + 128] * y[:, at : at + 128] for at in range(0, y.shape[1], 128))

    steady = (last >= 0) & (c < chunks)
    if lags[0] == 1:
        steady = c < 0

    @pl.when(c == 0)
    def _():
        _greet(left, right)
        square_s[...] = jnp.zeros_like(square_s)

    @pl.when((c < chunks) & jnp.logical_not(steady))
    def _():
        make()

        @pl.when(c == 0)
        def _():
            _met()

        set_off()

    if lags[0] > 1:

        @pl.when(steady)
        def _():
            for way in (0, 1):
                far_copy(way, on).wait_recv()
                to_copy(way, last).wait_recv()
            for way in (0, 1):
                pass_on(way, on)
            finish()
            make()
            for way in (0, 1):
                to_copy(way, on).start()
            set_off()

        @pl.when(c == chunks - 1)
        def _():
            pass_through(c - 1)

    @pl.when((on >= 0) & (on < chunks - (lags[0] - 1)) & jnp.logical_not(steady) if lags[0] == 1 else (on >= 0) & (c < lags[1]))
    def _():
        pass_through(on)

    if lags[0] > 1:

        @pl.when(c == chunks)
        def _():
            pass_through(c - 1)

    @pl.when((last >= 0) & jnp.logical_not(steady))
    def _():
        for way in (0, 1):
            to_copy(way, last).wait_recv()
        finish()

    @pl.when(c == pl.num_programs(0) - 1)
    def _():
        mean = square_s[...].sum(-1, keepdims=True) / (chunks * x_ref.shape[1])
        scale_ref[...] = jnp.broadcast_to(lax.rsqrt(mean + 1e-6), scale_ref.shape)

        def one(j, _):
            for way in (0, 1):
                far_copy(way, j).wait_send()
                to_copy(way, j).wait_send()

        lax.fori_loop(0, chunks, one, None)


def scatter(n, a, w, x, wide, lags, ident, name):
    (tokens, depth), width = a.shape, w.shape[1]
    rows = tokens // n
    wide = _fit(width, wide)
    chunks = width // wide
    done = pl.BlockSpec((rows, wide), lambda c: (0, jnp.maximum(c - lags[1], 0)))
    return pl.pallas_call(
        functools.partial(_scatter, n, chunks, lags),
        grid=(chunks + lags[1],),
        in_specs=[_whole(a.shape), pl.BlockSpec((depth, wide), lambda c: (0, jnp.minimum(c, chunks - 1))), done],
        out_specs=[done, _whole((rows, 128))],
        out_shape=[jax.ShapeDtypeStruct((rows, width), BF16), jax.ShapeDtypeStruct((rows, 128), F32)],
        scratch_shapes=[
            pltpu.VMEM((rows, 128), F32),
            pltpu.VMEM((lags[1] + 1, tokens, wide), F32),
            pltpu.VMEM((chunks, 2, rows // 2, wide), BF16),
            pltpu.VMEM((2, chunks, rows, wide), BF16),
            pltpu.VMEM((chunks, 2, rows // 2, wide), BF16),
            pltpu.VMEM((2, chunks, rows, wide), BF16),
            pltpu.SemaphoreType.DMA((4, chunks)),
            pltpu.SemaphoreType.DMA((4, chunks)),
        ],
        compiler_params=pltpu.CompilerParams(collective_id=ident, has_side_effects=True, vmem_limit_bytes=VMEM, dimension_semantics=("arbitrary",)),
        cost_estimate=pl.CostEstimate(flops=2 * tokens * width * depth, transcendentals=0, bytes_accessed=2 * width * depth),
        name=name,
    )(a, w, x)


def _attend(heads, q_ref, k_ref, v_ref, o_ref, v_s):
    tokens = q_ref.shape[0]
    e = HEAD**-0.5 * LOG2E
    v_s[:, :HEAD] = v_ref[...]
    v_s[:, HEAD:] = jnp.ones((tokens, HEAD), BF16)
    size, cols = HEAD, [slice(i * HEAD, (i + 1) * HEAD) for i in range(heads)]
    shape = (heads * size, size)
    seen = lax.rem(lax.broadcasted_iota(jnp.int32, shape, 0), size) >= lax.broadcasted_iota(jnp.int32, shape, 1)
    for at in range(0, tokens, size):
        end = at + size
        q = jnp.concatenate([q_ref[at:end, c] for c in cols], axis=0)
        s = lax.dot_general(q, k_ref[:end, :], (((1,), (1,)), ((), ())), preferred_element_type=F32)
        last = jnp.where(seen, s[:, at:], -jnp.inf)
        s = jnp.concatenate([s[:, :at], last], axis=1) if at else last
        top = s.max(-1, keepdims=True)
        p = jnp.exp2((s - top) * e).astype(BF16)
        mix = _dot(p, v_s[:end, :])
        out = (mix[:, :HEAD] / mix[:, HEAD:]).astype(BF16)
        for i, c in enumerate(cols):
            o_ref[at:end, c] = out[i * size : (i + 1) * size]


def attention(q, k, v, heads=4):
    tokens, width = q.shape
    per = width // k.shape[1] // heads
    key = pl.BlockSpec((tokens, HEAD), lambda i: (0, i // per))
    query = pl.BlockSpec((tokens, heads * HEAD), lambda i: (0, i))
    return pl.pallas_call(
        functools.partial(_attend, heads),
        grid=(width // HEAD // heads,),
        in_specs=[query, key, key],
        out_specs=query,
        out_shape=jax.ShapeDtypeStruct(q.shape, BF16),
        scratch_shapes=[pltpu.VMEM((tokens, 2 * HEAD), BF16)],
        compiler_params=pltpu.CompilerParams(dimension_semantics=("arbitrary",), vmem_limit_bytes=VMEM),
        cost_estimate=pl.CostEstimate(flops=4 * tokens * tokens * width, transcendentals=tokens * tokens * width // HEAD, bytes_accessed=4 * q.size),
        name="attention",
    )(q, k, v)


def rotation(tokens):
    half = HEAD // 2
    angle = np.arange(tokens, dtype=np.float32)[:, None] * np.float32(THETA) ** (-np.arange(half, dtype=np.float32) / np.float32(half))
    cos, sin = np.cos(angle), np.sin(angle)
    return np.concatenate([cos, cos], 1).astype(np.float32), np.concatenate([-sin, sin], 1).astype(np.float32)


def solution(mesh):
    n = mesh.shape["tp"]

    def step(x, gain_a, wq, wk, wv, wo, gain_m, w_gate, w_up, w_down):
        cos, sin = rotation(n * x.shape[0])
        q, k, v = project(n, x, gain_a, wq, wk, wv, jnp.asarray(cos), jnp.asarray(sin))
        h, scale = scatter(n, attention(q, k, v), wo, x, 512, (1, 2), 2, "attention_out")
        hidden = gate_up(n, h, scale, gain_m, w_gate, w_up)
        return scatter(n, hidden, w_down, h, 512, (2, 4), 3, "down")[0]

    tokens, columns, rows_of = P(("dp", "tp"), None), P(None, "tp"), P("tp", None)
    return jax.shard_map(
        step,
        mesh=mesh,
        in_specs=(tokens, P(None), columns, columns, columns, rows_of, P(None), columns, columns, rows_of),
        out_specs=tokens,
        check_vma=False,
    )
```
